32 devices in a mesh: py: 4 (over z), pz: 8 (over y, x, core).
Axes of the slice: x: 2, y: 2, z: 4, core: 2. Of those that a mesh axis runs over, the one named last changes fastest.
Arguments:
- field: bfloat16 [128, 128, 64, 256], P('py', 'pz'), may hold values from -60 to 60
- spectral_weights: bfloat16 [32, 32, 32, 2, 64, 64], P('py', 'pz'), may hold values from -0.5 to 0.5
- bypass_weight: bfloat16 [64, 64], replicated, may hold values from -0.75 to 0.75
Outputs:
- normalized: bfloat16 [128, 128, 64, 256], P('py', 'pz')
The draws below stay inside these ranges and needn't reach their ends.
All inputs are finite; a program needn't handle non-finite values.
Results may differ from the reference program's by a relative error of at most 0.0081.
Values may be sent and summed in bfloat16 or wider, within the bound.
A program may use at most 192 MiB of HBM per device.

```python
import math
import jax
import jax.numpy as jnp
from jax import lax

NX = 256
NY = 128
NZ = 128
C = 64
MODES = 32


def draw_field(key, part):
    noise_key, scale_key = jax.random.split(key)
    row_place = jnp.arange(NY, dtype=jnp.float32)[:, None, None, None] / NY
    column_place = jnp.arange(NZ, dtype=jnp.float32)[None, :, None, None] / NZ
    channel_scale = jnp.exp(jax.random.uniform(scale_key, (C,), jnp.float32, math.log(0.3), math.log(3.0)))
    channel_scale = channel_scale[None, None, :, None]
    noise_part = jnp.clip(jax.random.normal(noise_key, (NY, NZ, C, NX), jnp.float32), -6.0, 6.0)
    place_scale = jnp.sqrt((1.0 + 2.0 * row_place) * (1.0 + 2.0 * column_place))
    values = noise_part * channel_scale * place_scale
    return values.astype(jnp.bfloat16)


def block_levels(key, shape, pieces, smallest, top_value):
    factor_of, own = 1.0, jax.random.fold_in(key, 6)
    for dim, shards_of in pieces:
        draws = jnp.exp(jax.random.uniform(jax.random.fold_in(own, dim), (shards_of,), jnp.float32, smallest / len(pieces), top_value / len(pieces)))
        factor_of = factor_of * jnp.repeat(draws, shape[dim] // shards_of).reshape([-1 if axis == dim else 1 for axis in range(len(shape))])
    return factor_of


def bell_draw(own_key, shape, spread, bound, shards=(), kind=jnp.bfloat16):
    values = spread * jax.random.normal(own_key, shape, jnp.float32)
    if shards:
        values = values * block_levels(own_key, shape, shards, -0.22, 0.18)
    return jnp.clip(values, -bound, bound).astype(kind)


def setup_inputs(seed: int = 0) -> dict:
    arg_keys = jax.random.split(jax.random.key(seed), 4)
    return {
        "field": draw_field(jax.random.fold_in(arg_keys[3], 71), 0),
        "spectral_weights": bell_draw(arg_keys[1], (MODES, MODES, MODES, 2, C, C), (2 * C) ** -0.5, 0.5, ((0, 4), (1, 8))),
        "bypass_weight": bell_draw(arg_keys[2], (C, C), C ** -0.5, 0.75),
    }


def mode_frequencies(mode_count):
    ordinal = jnp.arange(mode_count, dtype=jnp.float32)
    return jnp.where(ordinal < mode_count // 2, ordinal, ordinal - mode_count)

def phase_angles(length, mode_count):
    points = jnp.arange(length, dtype=jnp.float32)
    return 2.0 * math.pi / length * points[:, None] * mode_frequencies(mode_count)[None, :]

def real_forward(length, mode_count):
    angles = phase_angles(length, mode_count)
    matrix = jnp.stack([jnp.cos(angles), -jnp.sin(angles)], axis=2).reshape(length, 2 * mode_count)
    return (matrix / math.sqrt(length)).astype(jnp.bfloat16)

def complex_forward(length, mode_count):
    angles = phase_angles(length, mode_count)
    cosine = jnp.cos(angles)
    sine_part = jnp.sin(angles)
    from_real = jnp.stack([cosine, -sine_part], axis=2)
    from_imag = jnp.stack([sine_part, cosine], axis=2)
    return (jnp.stack([from_real, from_imag], axis=1) / math.sqrt(length)).astype(jnp.bfloat16)

def complex_inverse(length, mode_count):
    angles = phase_angles(length, mode_count).T
    cosine = jnp.cos(angles)
    sine_part = jnp.sin(angles)
    from_real = jnp.stack([cosine, sine_part], axis=2)
    from_imag = jnp.stack([-sine_part, cosine], axis=2)
    return (jnp.stack([from_real, from_imag], axis=1) / math.sqrt(mode_count)).astype(jnp.bfloat16)

def real_inverse(length, mode_count):
    angles = phase_angles(length, mode_count).T
    matrix = jnp.stack([jnp.cos(angles), -jnp.sin(angles)], axis=1).reshape(2 * mode_count, length)
    return (matrix / math.sqrt(mode_count)).astype(jnp.bfloat16)

def mix_modes(spectrum, weights):
    real_in = spectrum[..., 0].astype(jnp.float32)
    imag_in = spectrum[..., 1].astype(jnp.float32)
    real_w = weights[:, :, :, 0].astype(jnp.float32)
    imag_w = weights[:, :, :, 1].astype(jnp.float32)

    def product(operand, coefficient):
        return jnp.einsum('cabk,abkco->oabk', operand, coefficient)
    real_out = product(real_in, real_w) - product(imag_in, imag_w)
    imag_out = product(real_in, imag_w) + product(imag_in, real_w)
    return jnp.stack([real_out, imag_out], axis=-1).astype(jnp.bfloat16)

def reference(field, spectral_weights, bypass_weight):
    row_table = real_forward(NX, MODES)

    def first_pass(plane):
        flat = jnp.dot(plane.reshape(NZ * C, NX), row_table, preferred_element_type=jnp.float32)
        return flat.reshape(NZ, C, 2 * MODES).astype(jnp.bfloat16)
    row_modes = lax.map(first_pass, field)
    paired = row_modes.reshape(NY, NZ, C, MODES, 2).astype(jnp.float32)
    plane_modes = jnp.einsum('yzcmp,ypkq->zcmkq', paired, complex_forward(NY, MODES).astype(jnp.float32)).astype(jnp.bfloat16)
    spectrum = jnp.einsum('zcakp,zpjq->cakjq', plane_modes.astype(jnp.float32), complex_forward(NZ, MODES).astype(jnp.float32)).astype(jnp.bfloat16)
    mixed_modes = mix_modes(spectrum, spectral_weights)
    column_back = jnp.einsum('oabkp,kpzq->zoabq', mixed_modes.astype(jnp.float32), complex_inverse(NZ, MODES).astype(jnp.float32)).astype(jnp.bfloat16)
    plane_back = jnp.einsum('zoakp,kpyq->yzoaq', column_back.astype(jnp.float32), complex_inverse(NY, MODES).astype(jnp.float32)).astype(jnp.bfloat16)
    inverse_table = real_inverse(NX, MODES)
    mixing = bypass_weight.astype(jnp.float32)

    def activated_plane(planes):
        plane, coefficients = planes
        spectral = jnp.dot(coefficients.reshape(NZ * C, 2 * MODES), inverse_table, preferred_element_type=jnp.float32).reshape(NZ, C, NX)
        bypass = jnp.einsum('zcx,co->zox', plane.astype(jnp.float32), mixing)
        return jax.nn.gelu(spectral + bypass, approximate=True)
    entries = NX * NY * NZ * C

    def plane_total(planes):
        return jnp.sum(activated_plane(planes))
    field_mean = jnp.sum(lax.map(plane_total, (field, plane_back))) / entries

    def plane_spread(planes):
        return jnp.sum(jnp.square(activated_plane(planes) - field_mean))
    field_var = jnp.sum(lax.map(plane_spread, (field, plane_back))) / entries
    scaling = lax.rsqrt(field_var + 1e-05)

    def plane_output(planes):
        return ((activated_plane(planes) - field_mean) * scaling).astype(jnp.bfloat16)
    return lax.map(plane_output, (field, plane_back))
```

```python
import functools
import math

import jax
import jax.numpy as jnp
import numpy as np
from jax import lax
from jax.experimental import pallas as pl
from jax.experimental.pallas import tpu as pltpu
from jax.sharding import PartitionSpec as P

NX = 256
NY = 128
NZ = 128
C = 64
MODES = 32


def mode_frequencies(mode_count):
    ordinal = jnp.arange(mode_count, dtype=jnp.float32)
    return jnp.where(ordinal < mode_count // 2, ordinal, ordinal - mode_count)


def phase_angles(length, mode_count):
    points = jnp.arange(length, dtype=jnp.float32)
    return 2.0 * math.pi / length * points[:, None] * mode_frequencies(mode_count)[None, :]


def real_forward(length, mode_count):
    angles = phase_angles(length, mode_count)
    matrix = jnp.stack([jnp.cos(angles), -jnp.sin(angles)], axis=2).reshape(length, 2 * mode_count)
    return (matrix / math.sqrt(length)).astype(jnp.bfloat16)


def complex_forward(length, mode_count):
    angles = phase_angles(length, mode_count)
    cosine = jnp.cos(angles)
    sine_part = jnp.sin(angles)
    from_real = jnp.stack([cosine, -sine_part], axis=2)
    from_imag = jnp.stack([sine_part, cosine], axis=2)
    return (jnp.stack([from_real, from_imag], axis=1) / math.sqrt(length)).astype(jnp.bfloat16)


def complex_inverse(length, mode_count):
    angles = phase_angles(length, mode_count).T
    cosine = jnp.cos(angles)
    sine_part = jnp.sin(angles)
    from_real = jnp.stack([cosine, sine_part], axis=2)
    from_imag = jnp.stack([-sine_part, cosine], axis=2)
    return (jnp.stack([from_real, from_imag], axis=1) / math.sqrt(mode_count)).astype(jnp.bfloat16)


def real_inverse(length, mode_count):
    angles = phase_angles(length, mode_count).T
    matrix = jnp.stack([jnp.cos(angles), -jnp.sin(angles)], axis=1).reshape(2 * mode_count, length)
    return (matrix / math.sqrt(mode_count)).astype(jnp.bfloat16)


def mix_modes(spectrum, weights):
    real_in = spectrum[..., 0]
    imag_in = spectrum[..., 1]
    real_w = weights[:, :, :, 0]
    imag_w = weights[:, :, :, 1]

    def product(operand, coefficient):
        return jnp.einsum(
            "cabk,abkco->oabk", operand, coefficient, preferred_element_type=jnp.float32
        )

    real_out = product(real_in, real_w) - product(imag_in, imag_w)
    imag_out = product(real_in, imag_w) + product(imag_in, real_w)
    return jnp.stack([real_out, imag_out], axis=-1).astype(jnp.bfloat16)


def plain_layer(field, spectral_weights, bypass_weight):
    row_table = real_forward(NX, MODES)
    forward_plane = complex_forward(NY, MODES)
    forward_column = complex_forward(NZ, MODES)
    inverse_column = complex_inverse(NZ, MODES)
    inverse_plane = complex_inverse(NY, MODES)
    inverse_row = real_inverse(NX, MODES)
    flat = jnp.dot(field.reshape(-1, NX), row_table, preferred_element_type=jnp.float32)
    row_modes = flat.reshape(field.shape[:3] + (2 * MODES,)).astype(jnp.bfloat16)
    incoming = lax.all_to_all(row_modes, "py", split_axis=3, concat_axis=0, tiled=True)
    paired = incoming.reshape(incoming.shape[:3] + (-1, 2))
    plane_modes = jnp.einsum(
        "yzcmp,ypkq->zcmkq", paired, forward_plane, preferred_element_type=jnp.float32
    ).astype(jnp.bfloat16)
    plane_modes = plane_modes.reshape(plane_modes.shape[:3] + (-1,))
    incoming = lax.all_to_all(plane_modes, "pz", split_axis=3, concat_axis=0, tiled=True)
    paired = incoming.reshape(incoming.shape[:3] + (-1, 2))
    spectrum = jnp.einsum(
        "zcakp,zpjq->cakjq", paired, forward_column, preferred_element_type=jnp.float32
    ).astype(jnp.bfloat16)
    mixed_modes = mix_modes(spectrum, spectral_weights)
    column_back = jnp.einsum(
        "oabkp,kpzq->zoabq", mixed_modes, inverse_column, preferred_element_type=jnp.float32
    ).astype(jnp.bfloat16)
    column_back = column_back.reshape(column_back.shape[:3] + (-1,))
    incoming = lax.all_to_all(column_back, "pz", split_axis=0, concat_axis=3, tiled=True)
    paired = incoming.reshape(incoming.shape[:3] + (-1, 2))
    plane_back = jnp.einsum(
        "zcakp,kpyq->yzcaq", paired, inverse_plane, preferred_element_type=jnp.float32
    ).astype(jnp.bfloat16)
    plane_back = plane_back.reshape(plane_back.shape[:3] + (-1,))
    incoming = lax.all_to_all(plane_back, "py", split_axis=0, concat_axis=3, tiled=True)
    points = jnp.dot(
        incoming.reshape(-1, 2 * MODES), inverse_row, preferred_element_type=jnp.float32
    )
    spectral = points.reshape(incoming.shape[:3] + (NX,))
    bypass = jnp.einsum("yzcx,co->yzox", field, bypass_weight, preferred_element_type=jnp.float32)
    activated = jax.nn.gelu(spectral + bypass, approximate=True)
    entries = NX * NY * NZ * C
    summed, squared = lax.psum((jnp.sum(activated), jnp.sum(activated * activated)), ("py", "pz"))
    field_mean = summed / entries
    field_var = squared / entries - field_mean * field_mean
    return ((activated - field_mean) * lax.rsqrt(field_var + 1e-05)).astype(jnp.bfloat16)


def np_angles(length, mode_count):
    ordinal = np.arange(mode_count, dtype=np.float32)
    frequency = np.where(ordinal < mode_count // 2, ordinal, ordinal - mode_count).astype(np.float32)
    points = np.arange(length, dtype=np.float32)
    scale = np.float32(2.0 * math.pi / length)
    return scale * points[:, None] * frequency[None, :]


def np_tables(ny, nz, nx, modes):
    angles = np_angles(nx, modes)
    row = np.stack([np.cos(angles), -np.sin(angles)], axis=2).reshape(nx, 2 * modes)
    row = (row / np.float32(math.sqrt(nx))).T
    inverse_row = np.stack([np.cos(angles.T), -np.sin(angles.T)], axis=1).reshape(2 * modes, nx)
    inverse_row = inverse_row / np.float32(math.sqrt(modes))

    def forward(length):
        a = np_angles(length, modes)
        c, s = np.cos(a), np.sin(a)
        table = np.stack([np.stack([c, -s], axis=2), np.stack([s, c], axis=2)], axis=1)
        return table / np.float32(math.sqrt(length))

    def inverse(length):
        a = np_angles(length, modes).T
        c, s = np.cos(a), np.sin(a)
        table = np.stack([np.stack([c, s], axis=2), np.stack([-s, c], axis=2)], axis=1)
        return table / np.float32(math.sqrt(modes))

    column = forward(nz).transpose(2, 3, 1, 0).reshape(2 * modes, 2 * nz)
    plane = forward(ny).reshape(ny // 2, 2, 2, modes, 2).transpose(1, 3, 4, 2, 0)
    plane = plane.reshape(4 * modes, ny)
    back_plane = inverse(ny).reshape(modes, 2, ny // 2, 2, 2).transpose(4, 2, 3, 0, 1)
    back_plane = back_plane.reshape(ny, 4 * modes)
    back_column = inverse(nz).transpose(3, 2, 0, 1).reshape(2 * nz, 2 * modes)
    tables = (row, column, plane, back_plane, back_column, inverse_row)
    return tuple(np.asarray(t, np.float32).astype(jnp.bfloat16) for t in tables)


MESH_ID = pl.DeviceIdType.MESH


def greet(axis, size, me):
    barrier = pltpu.get_barrier_semaphore()
    for step in range(1, size):
        pl.semaphore_signal(
            barrier, inc=1, device_id={axis: lax.rem(me + step, size)}, device_id_type=MESH_ID
        )
    pl.semaphore_wait(barrier, size - 1)


def send_pieces(axis, size, me, source_of, target, send_sem, recv_sem):
    for step in range(1, size):
        peer = lax.rem(me + step, size)
        pltpu.make_async_remote_copy(
            src_ref=source_of(peer),
            dst_ref=target,
            send_sem=send_sem.at[step],
            recv_sem=recv_sem.at[step],
            device_id={axis: peer},
            device_id_type=MESH_ID,
        ).start()
    pltpu.make_async_copy(source_of(me), target, send_sem.at[0]).start()


def wait_pieces(size, me, source_of, place_of, send_sem, recv_sem):
    for step in range(1, size):
        sent = source_of(lax.rem(me + step, size))
        pltpu.make_async_copy(sent, sent, send_sem.at[step]).wait()
        place = place_of(lax.rem(me + size - step, size))
        pltpu.make_async_copy(place, place, recv_sem.at[step]).wait()
    own = source_of(me)
    pltpu.make_async_copy(own, own, send_sem.at[0]).wait()


def dot(a, b):
    return jnp.dot(a, b, preferred_element_type=jnp.float32)


NT = (((1,), (1,)), ((), ()))
TN = (((0,), (0,)), ((), ()))


def row_kernel(size, steps, field_ref, table_ref, out_ref, held, wide, send_sem, recv_sem):
    step = pl.program_id(0)
    me = lax.axis_index("pz")
    rows, zs, cs, nx = field_ref.shape
    modes2 = table_ref.shape[0]
    group = modes2 // size

    @pl.when(step == 0)
    def _():
        greet("pz", size, me)

    for z in range(zs):
        block = field_ref[:, z].reshape(rows * cs, nx)
        wide[pl.ds(z, modes2, stride=zs), :] = lax.dot_general(
            table_ref[...], block, NT, preferred_element_type=jnp.float32
        )
    held[step] = wide[...].astype(jnp.bfloat16).reshape(modes2, zs, rows * cs)

    send_pieces(
        "pz", size, me,
        lambda peer: held.at[step, pl.ds(peer * group, group)],
        out_ref.at[step, :, pl.ds(pl.multiple_of(me * zs, zs), zs)],
        send_sem, recv_sem,
    )

    @pl.when(step == steps - 1)
    def _():
        wait_pieces(
            size, me,
            lambda peer: held.at[:, pl.ds(peer * group, group)],
            lambda peer: out_ref.at[:, :, pl.ds(pl.multiple_of(peer * zs, zs), zs)],
            send_sem, recv_sem,
        )


def column_kernel(size, steps, in_ref, table_ref, out_ref, held, wide, send_sem, recv_sem):
    step = pl.program_id(0)
    me = lax.axis_index("py")
    modes2 = table_ref.shape[0]
    kxs, _, _, lanes = held.shape
    nz = in_ref.shape[2]
    group = modes2 // size

    @pl.when(step == 0)
    def _():
        greet("py", size, me)

    for kx in range(kxs):
        rhs = in_ref[0, 2 * kx : 2 * kx + 2].reshape(2 * nz, lanes)
        wide[pl.ds(kx * modes2 * steps + step, modes2, stride=steps), :] = dot(table_ref[...], rhs)

    @pl.when(step == steps - 1)
    def _():
        for kx in range(kxs):
            part = wide[kx * modes2 * steps : (kx + 1) * modes2 * steps, :]
            held[kx] = part.astype(jnp.bfloat16).reshape(modes2, steps, lanes)
        source_of = lambda peer: held.at[:, pl.ds(peer * group, group)]
        place_of = lambda peer: out_ref.at[:, :, pl.ds(pl.multiple_of(peer * steps, steps), steps)]
        send_pieces("py", size, me, source_of, place_of(me), send_sem, recv_sem)
        wait_pieces(size, me, source_of, place_of, send_sem, recv_sem)


def plane_kernel(in_ref, table_ref, out_ref):
    _, kzs2, ys, lanes = in_ref.shape
    half = lanes // 2
    modes2 = table_ref.shape[0] // 2
    for kz in range(kzs2 // 2):
        rhs = in_ref[0, 2 * kz : 2 * kz + 2].reshape(2 * ys, lanes)
        both = dot(table_ref[...], rhs)
        out_ref[0, kz] = (both[:modes2, :half] + both[modes2:, half:]).astype(jnp.bfloat16)


def back_plane_kernel(size, in_ref, table_ref, out_ref, held, wide, send_sem, recv_sem):
    me = lax.axis_index("py")
    kxs, kzs, modes2, cs = in_ref.shape
    _, _, steps, group, lanes = held.shape
    half = size * steps
    greet("py", size, me)
    zero = jnp.zeros((modes2, cs), jnp.bfloat16)
    for kx in range(kxs):
        for kz in range(kzs):
            piece = in_ref[kx, kz]
            rhs = jnp.concatenate(
                [jnp.concatenate([piece, zero], 1), jnp.concatenate([zero, piece], 1)], 0
            )
            val = dot(table_ref[...], rhs)
            for q in range(2):
                for peer in range(size):
                    start = q * half + peer * steps
                    first = (peer * kxs + kx) * steps * group + 2 * kz + q
                    wide[pl.ds(first, steps, stride=group), :] = val[start : start + steps]
    for peer in range(size):
        rows = kxs * steps * group
        part = wide[peer * rows : (peer + 1) * rows, :].astype(jnp.bfloat16)
        held[peer] = part.reshape(kxs, steps, group, lanes)
    source_of = lambda peer: held.at[peer]
    place_of = lambda peer: out_ref.at[:, :, pl.ds(pl.multiple_of(peer * group, group), group)]
    send_pieces("py", size, me, source_of, place_of(me), send_sem, recv_sem)
    wait_pieces(size, me, source_of, place_of, send_sem, recv_sem)


def back_column_kernel(size, steps, in_ref, table_ref, out_ref, held, wide, send_sem, recv_sem):
    step = pl.program_id(0)
    me = lax.axis_index("pz")
    kxs = in_ref.shape[0]
    _, nz, group, lanes = held.shape
    zs = nz // size

    @pl.when(step == 0)
    def _():
        greet("pz", size, me)

    for kx in range(kxs):
        val = dot(table_ref[...], in_ref[kx, 0])
        for q in range(2):
            wide[pl.ds(2 * kx + q, nz, stride=group), :] = val[q * nz : (q + 1) * nz]
    held[step] = wide[...].astype(jnp.bfloat16).reshape(nz, group, lanes)

    send_pieces(
        "pz", size, me,
        lambda peer: held.at[step, pl.ds(peer * zs, zs)],
        out_ref.at[step, :, pl.ds(pl.multiple_of(me * group, group), group)],
        send_sem, recv_sem,
    )

    @pl.when(step == steps - 1)
    def _():
        wait_pieces(
            size, me,
            lambda peer: held.at[:, pl.ds(peer * zs, zs)],
            lambda peer: out_ref.at[:, :, pl.ds(pl.multiple_of(peer * group, group), group)],
            send_sem, recv_sem,
        )


def point_kernel(in_ref, field_ref, table_ref, mix_ref, act_ref, sums_ref):
    rows, zs, cs, nx = field_ref.shape

    @pl.when(pl.program_id(0) == 0)
    def _():
        sums_ref[...] = jnp.zeros_like(sums_ref)

    for z in range(zs):
        spectral = lax.dot_general(
            in_ref[0, z], table_ref[...], TN, preferred_element_type=jnp.float32
        )
        v = spectral + dot(mix_ref[...], field_ref[:, z].reshape(rows * cs, nx))
        inner = math.sqrt(2.0 / math.pi) * (v + 0.044715 * (v * v * v))
        act = 0.5 * v * (1.0 + jnp.tanh(inner))
        act_ref[:, z] = act.astype(jnp.bfloat16).reshape(rows, cs, nx)
        tall = act.reshape(-1, 8, nx)
        sums_ref[0] += jnp.sum(tall, axis=0)
        sums_ref[1] += jnp.sum(tall * tall, axis=0)


def sum_kernel(py, pz, sums_ref, out_ref, mine, held, send_sem, recv_sem):
    count = py * pz
    me = lax.axis_index("py") * pz + lax.axis_index("pz")
    peers = []
    for step in range(1, count):
        peer = lax.rem(me + step, count)
        peers.append({"py": lax.div(peer, pz), "pz": lax.rem(peer, pz)})
    barrier = pltpu.get_barrier_semaphore()
    for peer in peers:
        pl.semaphore_signal(barrier, inc=1, device_id=peer, device_id_type=MESH_ID)
    for k in range(2):
        total = jnp.sum(sums_ref[k], axis=0, keepdims=True)
        total = sum(total[:, i : i + 128] for i in range(0, total.shape[1], 128))
        mine[4 * k : 4 * k + 4, :] = jnp.broadcast_to(total, (4, 128))
    pl.semaphore_wait(barrier, count - 1)
    copies = []
    for step, peer in enumerate(peers):
        copy = pltpu.make_async_remote_copy(
            src_ref=mine, dst_ref=held.at[step], send_sem=send_sem.at[step],
            recv_sem=recv_sem.at[step], device_id=peer, device_id_type=MESH_ID,
        )
        copy.start()
        copies.append(copy)
    for copy in copies:
        copy.wait()
    total = mine[...] + jnp.sum(held[...], axis=0)
    out_ref[...] = total


def scale_kernel(entries, total_ref, act_ref, out_ref):
    mean = jnp.sum(total_ref[0:1, :], keepdims=True)[:1, :1] / entries
    square = jnp.sum(total_ref[4:5, :], keepdims=True)[:1, :1] / entries
    scale = lax.rsqrt(square - mean * mean + 1e-05)
    rows, zs, cs, nx = act_ref.shape
    for z in range(zs):
        v = act_ref[:, z].reshape(rows * cs, nx).astype(jnp.float32)
        out_ref[:, z] = ((v - mean) * scale).astype(jnp.bfloat16).reshape(rows, cs, nx)


def exchange_params(number):
    return pltpu.CompilerParams(
        collective_id=number, has_side_effects=True, vmem_limit_bytes=48 * 1024 * 1024
    )


ANY = pl.BlockSpec(memory_space=pl.ANY)
WHOLE = pl.BlockSpec(memory_space=pltpu.VMEM)


def on_device(py, pz, field, spectral_weights, bypass_weight):
    ys, zs, cs, nx = field.shape
    modes = spectral_weights.shape[2]
    ny, nz = ys * py, zs * pz
    steps, lanes, modes2 = ys // 2, 2 * cs, 2 * modes
    kxs, kys, kzs = modes // pz, modes // pz, modes // py
    aligned = lanes % 128 == 0 and zs % 16 == 0 and steps % 16 == 0 and kzs % 8 == 0
    if not aligned or kxs % 4 or modes % 32:
        return plain_layer(field, spectral_weights, bypass_weight)
    row, column, plane, back_plane, back_column, inverse_row = np_tables(ny, nz, nx, modes)
    bf16, f32 = jnp.bfloat16, jnp.float32
    vmem, dma = pltpu.VMEM, pltpu.SemaphoreType.DMA
    table = lambda t: pl.BlockSpec(t.shape, lambda i: (0,) * t.ndim)
    field_block = pl.BlockSpec((2, zs, cs, nx), lambda i: (i, 0, 0, 0))

    z_rows = pl.pallas_call(
        functools.partial(row_kernel, pz, steps),
        grid=(steps,),
        out_shape=jax.ShapeDtypeStruct((steps, 2 * kxs, nz, lanes), bf16),
        in_specs=[field_block, table(row)],
        out_specs=ANY,
        scratch_shapes=[
            vmem((steps, modes2, zs, lanes), bf16), vmem((modes2 * zs, lanes), f32),
            dma((pz,)), dma((pz,)),
        ],
        compiler_params=exchange_params(1),
        name="row_modes",
    )(field, row)

    y_rows = pl.pallas_call(
        functools.partial(column_kernel, py, steps),
        grid=(steps,),
        out_shape=jax.ShapeDtypeStruct((kxs, 2 * kzs, ny // 2, lanes), bf16),
        in_specs=[pl.BlockSpec((1, 2 * kxs, nz, lanes), lambda i: (i, 0, 0, 0)), table(column)],
        out_specs=ANY,
        scratch_shapes=[
            vmem((kxs, modes2, steps, lanes), bf16), vmem((kxs * modes2 * steps, lanes), f32),
            dma((py,)), dma((py,)),
        ],
        compiler_params=exchange_params(2),
        name="column_modes",
    )(z_rows, column)

    spectrum = pl.pallas_call(
        plane_kernel,
        grid=(kxs,),
        out_shape=jax.ShapeDtypeStruct((kxs, kzs, modes2, cs), bf16),
        in_specs=[pl.BlockSpec((1, 2 * kzs, ny // 2, lanes), lambda i: (i, 0, 0, 0)), table(plane)],
        out_specs=pl.BlockSpec((1, kzs, modes2, cs), lambda i: (i, 0, 0, 0)),
        name="plane_modes",
    )(y_rows, plane)

    moved = spectrum.reshape(kxs, kzs, modes, 2 * cs)
    moved = lax.all_to_all(moved, "pz", split_axis=2, concat_axis=0, tiled=True)
    moved = lax.all_to_all(moved, "py", split_axis=0, concat_axis=1, tiled=True)
    moved = moved.transpose(0, 2, 1, 3)
    real, imag = moved[..., :cs], moved[..., cs:]
    lhs = jnp.stack([moved, jnp.concatenate([imag, real], -1)], axis=3)
    sign = np.ones((2, 2 * cs), np.float32)
    sign[0, cs:] = -1.0
    lhs = lhs * jnp.asarray(sign, bf16)
    stacked = spectral_weights.reshape(spectral_weights.shape[:3] + (2 * cs, cs))
    mixed = jnp.einsum("abkqi,abkio->abkqo", lhs, stacked, preferred_element_type=f32).astype(bf16)
    mixed = mixed.reshape(mixed.shape[:3] + (2 * cs,))
    mixed = lax.all_to_all(mixed, "py", split_axis=2, concat_axis=0, tiled=True)
    mixed = lax.all_to_all(mixed, "pz", split_axis=0, concat_axis=1, tiled=True)
    mixed = mixed.transpose(0, 2, 1, 3).reshape(kxs, kzs, modes2, cs)

    kz_rows = pl.pallas_call(
        functools.partial(back_plane_kernel, py),
        out_shape=jax.ShapeDtypeStruct((kxs, steps, modes2, lanes), bf16),
        in_specs=[WHOLE, WHOLE],
        out_specs=ANY,
        scratch_shapes=[
            vmem((py, kxs, steps, 2 * kzs, lanes), bf16),
            vmem((py * kxs * steps * 2 * kzs, lanes), f32),
            dma((py,)), dma((py,)),
        ],
        compiler_params=exchange_params(3),
        name="plane_back",
    )(mixed, back_plane)

    kx_rows = pl.pallas_call(
        functools.partial(back_column_kernel, pz, steps),
        grid=(steps,),
        out_shape=jax.ShapeDtypeStruct((steps, zs, modes2, lanes), bf16),
        in_specs=[
            pl.BlockSpec((kxs, 1, modes2, lanes), lambda i: (0, i, 0, 0)), table(back_column),
        ],
        out_specs=ANY,
        scratch_shapes=[
            vmem((steps, nz, 2 * kxs, lanes), bf16), vmem((nz * 2 * kxs, lanes), f32),
            dma((pz,)), dma((pz,)),
        ],
        compiler_params=exchange_params(4),
        name="column_back",
    )(kz_rows, back_column)

    flipped = bypass_weight.T
    zero = jnp.zeros_like(flipped)
    mix = jnp.concatenate(
        [jnp.concatenate([flipped, zero], 1), jnp.concatenate([zero, flipped], 1)], 0
    )
    activated, sums = pl.pallas_call(
        point_kernel,
        grid=(steps,),
        out_shape=[
            jax.ShapeDtypeStruct(field.shape, bf16), jax.ShapeDtypeStruct((2, 8, nx), f32),
        ],
        in_specs=[
            pl.BlockSpec((1, zs, modes2, lanes), lambda i: (i, 0, 0, 0)),
            field_block, table(inverse_row), table(mix),
        ],
        out_specs=[field_block, pl.BlockSpec((2, 8, nx), lambda i: (0, 0, 0))],
        name="points",
    )(kx_rows, field, inverse_row, mix)

    count = py * pz
    total = pl.pallas_call(
        functools.partial(sum_kernel, py, pz),
        out_shape=jax.ShapeDtypeStruct((8, 128), f32),
        in_specs=[WHOLE],
        out_specs=WHOLE,
        scratch_shapes=[
            vmem((8, 128), f32), vmem((count - 1, 8, 128), f32), dma((count,)), dma((count,)),
        ],
        compiler_params=exchange_params(5),
        name="totals",
    )(sums)

    return pl.pallas_call(
        functools.partial(scale_kernel, float(ny * nz * cs * nx)),
        grid=(steps,),
        out_shape=jax.ShapeDtypeStruct(field.shape, bf16),
        in_specs=[pl.BlockSpec((8, 128), lambda i: (0, 0)), field_block],
        out_specs=field_block,
        name="normalize",
    )(total, activated)


def solution(mesh):
    in_specs = (P("py", "pz", None, None), P("py", "pz", None, None, None, None), P())
    out_specs = P("py", "pz", None, None)
    body = functools.partial(on_device, mesh.shape["py"], mesh.shape["pz"])
    return jax.shard_map(
        body, mesh=mesh, in_specs=in_specs, out_specs=out_specs, check_vma=False
    )
```
